32 devices in a mesh: shard: 8 (over y, x, core), width: 4 (over z).
Axes of the slice: x: 2, y: 2, z: 4, core: 2. Of those that a mesh axis runs over, the one named last changes fastest.
Arguments:
- w_up: bfloat16 [12288, 49152], P('shard', 'width'), may hold values from -0.078125 to 0.078125
- low_up: bfloat16 [12288, 64], P('shard'), may hold values from -0.0546875 to 0.0546875
- high_up: bfloat16 [64, 49152], P(None, 'width'), may hold values from -0.75 to 0.75
- norm_train: float32 [12288], P(('shard', 'width')), may hold values from 0.25 to 1.75
- norm_step: float32 [12288], P(('shard', 'width')), may hold values from -0.3 to 0.3
Outputs:
- serve_up: bfloat16 [12288, 49152], P(None, ('width', 'shard'))
- scale_up: float32 [49152], P(('width', 'shard'))
- serve_norm: bfloat16 [12288], replicated
The draws below stay inside these ranges and needn't reach their ends.
All inputs are finite; a program needn't handle non-finite values. Where the reference program divides by a largest or mean magnitude, that divisor is 1e-20 or more.
Results may differ from the reference program's by a relative error of at most 0.001.
Values may be sent and summed in bfloat16 or wider, within the bound.
A program may use at most 256 MiB of HBM per device.

```python
import jax
import jax.numpy as jnp

D_MODEL = 12288
D_INNER = 49152
RANK = 64


def raised(drawn, own_key, source, target, blocks, factor):
    def block_of(dim):
        return (jnp.arange(drawn.shape[dim]) // (drawn.shape[dim] // blocks)).reshape((-1,) + (1,) * (drawn.ndim - 1 - dim))

    one_side = jax.random.permutation(own_key, blocks)[block_of(target)]
    far = (block_of(target) + blocks // 2) % blocks
    return jnp.where((block_of(source) == one_side) | (block_of(source) == far), factor * drawn, drawn)


def block_levels(rng, extent, shards, smallest, high):
    def one(dim, parts):
        draws = jax.random.uniform(jax.random.fold_in(jax.random.fold_in(rng, 6), dim), (parts,), jnp.float32, smallest / len(shards), high / len(shards))
        return jnp.repeat(jnp.exp(draws), extent[dim] // parts).reshape((-1,) + (1,) * (len(extent) - dim - 1))

    gain = one(*shards[0])
    for cut in shards[1:]:
        gain = gain * one(*cut)
    return gain


def gaussian(rng, dims, width, reach, split=(), held_as=jnp.bfloat16):
    entries = width * jax.random.normal(rng, dims, jnp.float32)
    if split:
        entries = entries * block_levels(rng, dims, split, -0.22, 0.18)
    return jnp.clip(entries, -reach, reach).astype(held_as)


def heavy_noise(rng, extent, deviation, bound, cuts, heavy, held_as=jnp.bfloat16):
    result = deviation * jax.random.normal(rng, extent, jnp.float32)
    if cuts:
        result = result * block_levels(rng, extent, cuts, -0.22, 0.18)
    return jnp.clip(raised(result, jax.random.fold_in(rng, 3), *heavy), -bound, bound).astype(held_as)


def setup_inputs(seed: int = 0) -> dict:
    key_of = jax.random.split(jax.random.key(seed), 6)
    w_up = heavy_noise(key_of[0], (D_MODEL, D_INNER), D_MODEL ** -0.5, 0.078125, ((0, 8), (1, 4)), (0, 1, 8, 2.0))
    low_up = gaussian(key_of[1], (D_MODEL, RANK), D_MODEL ** -0.5, 0.0546875, ((0, 8),))
    high_up = gaussian(key_of[2], (RANK, D_INNER), RANK ** -0.5, 0.75, ((1, 4),))
    norm_train = jnp.clip(1.0 + 0.15 * jax.random.normal(key_of[3], (D_MODEL,), jnp.float32), 0.25, 1.75)
    norm_step = jnp.clip(jax.random.uniform(key_of[4], (D_MODEL,), jnp.float32, -0.3, 0.3) * block_levels(key_of[4], (D_MODEL,), ((0, 32),), -0.4, 0.0), -0.3, 0.3)
    return dict(w_up=w_up, low_up=low_up, high_up=high_up, norm_train=norm_train, norm_step=norm_step)


mix_rate = 0.5


def reference(w_up, low_up, high_up, norm_train, norm_step):
    fresh_up = w_up.astype(jnp.float32) + mix_rate * jnp.dot(low_up, high_up, preferred_element_type=jnp.float32)
    scale_up = jnp.sum(jnp.abs(fresh_up), axis=0) / D_MODEL
    serve_up = (fresh_up / scale_up).astype(jnp.bfloat16)
    serve_norm = (norm_train + norm_step).astype(jnp.bfloat16)
    return serve_up, scale_up, serve_norm
```

```python
import functools

import jax
import jax.numpy as jnp
from jax import lax
from jax.experimental import pallas as pl
from jax.experimental.pallas import tpu as pltpu
from jax.sharding import PartitionSpec as P

MESH = pl.DeviceIdType.MESH

mix_rate = 0.5


def tile_of(extent, most):
    for size in range(most, 0, -128):
        if extent % size == 0:
            return size
    return extent


def contract_first(a, b):
    return lax.dot_general(a, b, (((0,), (0,)), ((), ())), preferred_element_type=jnp.float32)


def exchange_kernel(
    n, depth, inner, w_ref, low_ref, high_ref, train_ref, step_ref,
    out_ref, mine_ref, scale_ref, norm_ref,
    small_ref, all_ref, parts_ref, high_own,
    big_send, big_recv, small_send, small_recv, far_send, far_recv,
    pair_send, pair_recv, part_send, part_recv, own_sem,
):
    me = lax.axis_index("shard")
    z = lax.axis_index("width")
    rows = w_ref.shape[0]
    rank = low_ref.shape[0]
    cols = out_ref.shape[1]
    part = rows // depth
    order = sorted(range(1, n), key=lambda k: (bin(k >> 1).count("1"), k))
    near = [k for k in order if bin(k >> 1).count("1") < 2]
    late = [k for k in order if bin(k >> 1).count("1") >= 2]
    chips = [k for k in order if k % 2 == 0]

    def columns(p):
        return pl.ds(pl.multiple_of(p * cols, cols), cols)

    def rows_of(p, q):
        return pl.ds(pl.multiple_of(p * rows + q * part, part), part)

    def big_copy(k, q):
        return pltpu.make_async_remote_copy(
            src_ref=w_ref.at[pl.ds(pl.multiple_of(q * part, part), part), columns(me ^ k)],
            dst_ref=out_ref.at[rows_of(me, q), :],
            send_sem=big_send.at[k, q], recv_sem=big_recv.at[k, q],
            device_id={"shard": me ^ k}, device_id_type=MESH,
        )

    def small_copy(k):
        return pltpu.make_async_remote_copy(
            src_ref=small_ref, dst_ref=all_ref.at[me, z],
            send_sem=small_send.at[k], recv_sem=small_recv.at[k],
            device_id={"shard": me ^ k}, device_id_type=MESH,
        )

    def far_copy(k, j):
        return pltpu.make_async_remote_copy(
            src_ref=all_ref.at[me ^ k, z], dst_ref=all_ref.at[me ^ k, z],
            send_sem=far_send.at[k, j], recv_sem=far_recv.at[k, j],
            device_id={"width": z ^ j}, device_id_type=MESH,
        )

    def pair_copy(k):
        return pltpu.make_async_remote_copy(
            src_ref=all_ref.at[me ^ k], dst_ref=all_ref.at[me ^ k],
            send_sem=pair_send.at[k], recv_sem=pair_recv.at[k],
            device_id={"shard": me ^ 1}, device_id_type=MESH,
        )

    def part_copy(k):
        return pltpu.make_async_remote_copy(
            src_ref=mine_ref.at[:, columns(me ^ k)], dst_ref=parts_ref.at[me],
            send_sem=part_send.at[k], recv_sem=part_recv.at[k],
            device_id={"shard": me ^ k}, device_id_type=MESH,
        )

    for q in range(1):
        for k in near:
            big_copy(k, q).start()

    own_block = pltpu.make_async_copy(
        w_ref.at[:, columns(me)], out_ref.at[pl.ds(pl.multiple_of(me * rows, rows), rows), :], own_sem.at[0]
    )
    own_block.start()
    own_high = pltpu.make_async_copy(high_ref.at[:, columns(me)], high_own, own_sem.at[1])
    own_high.start()

    for j in range(depth):
        @pl.when(z == j)
        def _():
            small_ref[:rank, :] = low_ref[:, j * part:(j + 1) * part] * jnp.bfloat16(mix_rate)
    gain = (train_ref[...] + step_ref[...]).astype(jnp.bfloat16)
    small_ref[rank:, :] = jnp.broadcast_to(gain, (8, part))

    tile = tile_of(w_ref.shape[1], 512)
    step = tile_of(rows, 256)

    def add_up(w_tile, high_tile, sum_tile):
        total = jnp.zeros((8, tile), jnp.float32)
        for r in range(0, rows, step):
            fresh = w_tile[r:r + step, :].astype(jnp.float32) + mix_rate * contract_first(
                low_ref[:, r:r + step], high_tile[...]
            )
            total = total + jnp.sum(jnp.abs(fresh).reshape(step // 8, 8, tile), axis=0)
        sum_tile[...] = jnp.sum(total, axis=0, keepdims=True)

    pltpu.emit_pipeline(
        add_up,
        grid=(w_ref.shape[1] // tile,),
        in_specs=[
            pl.BlockSpec((rows, tile), lambda j: (0, j)),
            pl.BlockSpec((rank, tile), lambda j: (0, j)),
        ],
        out_specs=[pl.BlockSpec((1, tile), lambda j: (0, j))],
    )(w_ref, high_ref, mine_ref)

    own_small = pltpu.make_async_copy(small_ref, all_ref.at[me, z], own_sem.at[2])
    own_small.start()
    own_part = pltpu.make_async_copy(mine_ref.at[:, columns(me)], parts_ref.at[me], own_sem.at[3])
    own_part.start()
    for k in chips:
        small_copy(k).start()
    for k in order:
        part_copy(k).start()
    for q in range(1, depth):
        for k in near:
            big_copy(k, q).start()
    for q in range(depth):
        for k in late:
            big_copy(k, q).start()

    own_small.wait()
    for k in [0] + chips:
        if k:
            small_copy(k).wait()
        for j in range(1, depth):
            far_copy(k, j).start()
    for k in [0] + chips:
        for j in range(1, depth):
            far_copy(k, j).wait()
        pair_copy(k).start()
    own_part.wait()
    for k in order:
        part_copy(k).wait()
    scale = jnp.sum(parts_ref[...], axis=0) / inner
    scale_ref[...] = scale
    inverse = 1.0 / scale
    for k in [0] + chips:
        pair_copy(k).wait()
    own_high.wait()
    own_block.wait()

    for d in range(n):
        for q in range(depth):
            i = d * depth + q
            norm_ref[i * 8:(i + 1) * 8, :] = all_ref[d, q, rank:, :]

    height = tile_of(part, 128)
    width = tile_of(cols, 512)

    def finish(k):
        d = me ^ k

        def piece(q, carry):
            if k:
                big_copy(k, q).wait_recv()
            for r in range(0, part, height):
                here = pl.ds(pl.multiple_of(d * rows + q * part + r, height), height)
                for c in range(0, cols, width):
                    fresh = out_ref[here, c:c + width].astype(jnp.float32) + contract_first(
                        all_ref[d, q, :rank, r:r + height], high_own[:, c:c + width]
                    )
                    out_ref[here, c:c + width] = (fresh * inverse[:, c:c + width]).astype(jnp.bfloat16)
            return carry

        return piece

    for k in [0] + near:
        lax.fori_loop(0, depth, finish(k), 0)
    late_pieces = [finish(k) for k in late]

    def late_round(q, carry):
        for piece in late_pieces:
            piece(q, carry)
        return carry

    lax.fori_loop(0, depth, late_round, 0)

    for q in range(depth):
        for k in order:
            big_copy(k, q).wait_send()


def put_kernel(held_ref, out_ref, sems):
    pieces = sems.shape[0]
    size = held_ref.shape[0] // pieces
    copies = [
        pltpu.make_async_copy(held_ref.at[i * size:(i + 1) * size, :], out_ref.at[i * size:(i + 1) * size, :], sems.at[i])
        for i in range(pieces)
    ]
    for copy in copies:
        copy.start()
    for copy in copies:
        copy.wait()


def tail_kernel(scale_in, norm_in, scale_ref, norm_ref):
    scale_ref[...] = scale_in[...].reshape(scale_ref.shape)
    part = norm_in.shape[1]
    for i in range(norm_in.shape[0] // 8):
        norm_ref[i * part:(i + 1) * part] = norm_in[i * 8:i * 8 + 1, :].reshape(part)


def solution(mesh):
    n, depth = mesh.shape["shard"], mesh.shape["width"]

    def per_device(w_up, low_up, high_up, norm_train, norm_step):
        rows, wide = w_up.shape
        rank = low_up.shape[1]
        cols = wide // n
        part = rows // depth
        any_spec = pl.BlockSpec(memory_space=pl.ANY)
        vmem_spec = pl.BlockSpec(memory_space=pltpu.VMEM)
        dma = pltpu.SemaphoreType.DMA
        held, _, scale, norm = pl.pallas_call(
            functools.partial(exchange_kernel, n, depth, n * rows),
            out_shape=(
                pltpu.VMEM((n * rows, cols), jnp.bfloat16),
                jax.ShapeDtypeStruct((1, wide), jnp.float32),
                jax.ShapeDtypeStruct((1, cols), jnp.float32),
                jax.ShapeDtypeStruct((n * depth * 8, part), jnp.bfloat16),
            ),
            in_specs=[any_spec, vmem_spec, any_spec, vmem_spec, vmem_spec],
            out_specs=(vmem_spec, any_spec, vmem_spec, vmem_spec),
            scratch_shapes=[
                pltpu.VMEM((rank + 8, part), jnp.bfloat16),
                pltpu.VMEM((n, depth, rank + 8, part), jnp.bfloat16),
                pltpu.VMEM((n, 1, cols), jnp.float32),
                pltpu.VMEM((rank, cols), jnp.bfloat16),
                dma((n, depth)), dma((n, depth)), dma((n,)), dma((n,)), dma((n, depth)), dma((n, depth)),
                dma((n,)), dma((n,)), dma((n,)), dma((n,)), dma((4,)),
            ],
            compiler_params=pltpu.CompilerParams(has_side_effects=True, vmem_limit_bytes=24 * 2**20),
            name="exchange",
        )(w_up, low_up.T, high_up, norm_train.reshape(1, part), norm_step.reshape(1, part))
        serve_up = pl.pallas_call(
            put_kernel,
            out_shape=jax.ShapeDtypeStruct((n * rows, cols), jnp.bfloat16),
            in_specs=[vmem_spec],
            out_specs=any_spec,
            scratch_shapes=[dma((8,))],
            compiler_params=pltpu.CompilerParams(vmem_limit_bytes=4 * 2**20),
            name="put",
        )(held)
        serve_up, scale, norm = lax.optimization_barrier((serve_up, scale, norm))
        scale_up, serve_norm = pl.pallas_call(
            tail_kernel,
            out_shape=(
                jax.ShapeDtypeStruct((cols,), jnp.float32),
                jax.ShapeDtypeStruct((n * rows,), jnp.bfloat16),
            ),
            in_specs=[vmem_spec, vmem_spec],
            out_specs=(vmem_spec, vmem_spec),
            compiler_params=pltpu.CompilerParams(vmem_limit_bytes=4 * 2**20),
            name="tail",
        )(scale, norm)
        return serve_up, scale_up, serve_norm

    placed = (
        P("shard", "width"),
        P("shard", None),
        P(None, "width"),
        P(("shard", "width")),
        P(("shard", "width")),
    )
    return jax.shard_map(
        per_device,
        mesh=mesh,
        in_specs=placed,
        out_specs=(P(None, ("width", "shard")), P(("width", "shard")), P()),
        check_vma=False,
    )
```

```python
import functools

import jax
import jax.numpy as jnp
from jax import lax
from jax.experimental import pallas as pl
from jax.experimental.pallas import tpu as pltpu
from jax.sharding import PartitionSpec as P

MESH = pl.DeviceIdType.MESH

mix_rate = 0.5


def tile_of(extent, most):
    for size in range(most, 0, -128):
        if extent % size == 0:
            return size
    return extent


def contract_first(a, b):
    return lax.dot_general(a, b, (((0,), (0,)), ((), ())), preferred_element_type=jnp.float32)


def exchange_kernel(
    n, depth, held_back, inner, w_ref, low_ref, high_ref, train_ref, step_ref,
    out_ref, mine_ref, scale_ref, norm_ref, low_late_ref,
    small_ref, all_ref, parts_ref, high_own,
    big_send, big_recv, small_send, small_recv, far_send, far_recv,
    pair_send, pair_recv, part_send, part_recv, unit_send, unit_recv, own_sem,
):
    me = lax.axis_index("shard")
    z = lax.axis_index("width")
    rows = w_ref.shape[0]
    rank = low_ref.shape[0]
    cols = out_ref.shape[1]
    part = rows // depth
    height = tile_of(part, 128)
    width = tile_of(cols, 512)
    units = rows // height
    far = n - 2
    order = sorted(range(1, n), key=lambda k: (bin(k >> 1).count("1"), k))
    near = [k for k in order if bin(k >> 1).count("1") < 2]
    late = [k for k in order if bin(k >> 1).count("1") >= 2 and k != far]
    chips = [k for k in order if k % 2 == 0]

    def columns(p):
        return pl.ds(pl.multiple_of(p * cols, cols), cols)

    def rows_of(p, q):
        return pl.ds(pl.multiple_of(p * rows + q * part, part), part)

    def big_copy(k, q):
        return pltpu.make_async_remote_copy(
            src_ref=w_ref.at[pl.ds(pl.multiple_of(q * part, part), part), columns(me ^ k)],
            dst_ref=out_ref.at[rows_of(me, q), :],
            send_sem=big_send.at[k, q], recv_sem=big_recv.at[k, q],
            device_id={"shard": me ^ k}, device_id_type=MESH,
        )

    def unit_copy(u):
        return pltpu.make_async_remote_copy(
            src_ref=w_ref.at[u * height:(u + 1) * height, columns(me ^ far)],
            dst_ref=out_ref.at[pl.ds(pl.multiple_of(me * rows + u * height, height), height), :],
            send_sem=unit_send.at[u], recv_sem=unit_recv.at[u],
            device_id={"shard": me ^ far}, device_id_type=MESH,
        )

    def small_copy(k):
        return pltpu.make_async_remote_copy(
            src_ref=small_ref, dst_ref=all_ref.at[me, z],
            send_sem=small_send.at[k], recv_sem=small_recv.at[k],
            device_id={"shard": me ^ k}, device_id_type=MESH,
        )

    def far_copy(k, j):
        return pltpu.make_async_remote_copy(
            src_ref=all_ref.at[me ^ k, z], dst_ref=all_ref.at[me ^ k, z],
            send_sem=far_send.at[k, j], recv_sem=far_recv.at[k, j],
            device_id={"width": z ^ j}, device_id_type=MESH,
        )

    def pair_copy(k):
        return pltpu.make_async_remote_copy(
            src_ref=all_ref.at[me ^ k], dst_ref=all_ref.at[me ^ k],
            send_sem=pair_send.at[k], recv_sem=pair_recv.at[k],
            device_id={"shard": me ^ 1}, device_id_type=MESH,
        )

    def part_copy(k):
        return pltpu.make_async_remote_copy(
            src_ref=mine_ref.at[:, columns(me ^ k)], dst_ref=parts_ref.at[me],
            send_sem=part_send.at[k], recv_sem=part_recv.at[k],
            device_id={"shard": me ^ k}, device_id_type=MESH,
        )

    barrier = pltpu.get_barrier_semaphore()
    for k in order:
        pl.semaphore_signal(barrier, inc=1, device_id={"shard": me ^ k}, device_id_type=MESH)
    for j in range(1, depth):
        pl.semaphore_signal(barrier, inc=1, device_id={"width": z ^ j}, device_id_type=MESH)
    pl.semaphore_wait(barrier, len(order) + depth - 1)

    for q in range(1):
        for k in near:
            big_copy(k, q).start()

    own_block = pltpu.make_async_copy(
        w_ref.at[:, columns(me)], out_ref.at[pl.ds(pl.multiple_of(me * rows, rows), rows), :], own_sem.at[0]
    )
    own_block.start()
    own_high = pltpu.make_async_copy(high_ref.at[:, columns(me)], high_own, own_sem.at[1])
    own_high.start()

    for j in range(depth):
        @pl.when(z == j)
        def _():
            small_ref[:rank, :] = low_ref[:, j * part:(j + 1) * part] * jnp.bfloat16(mix_rate)
    gain = (train_ref[...] + step_ref[...]).reshape(1, part)
    small_ref[rank:, :] = jnp.broadcast_to(gain, (8, part)).astype(jnp.bfloat16)

    tile = tile_of(w_ref.shape[1], 512)
    step = tile_of(rows, 256)

    def add_up(w_tile, high_tile, sum_tile):
        total = jnp.zeros((8, tile), jnp.float32)
        for r in range(0, rows, step):
            fresh = w_tile[r:r + step, :].astype(jnp.float32) + mix_rate * contract_first(
                low_ref[:, r:r + step], high_tile[...]
            )
            total = total + jnp.sum(jnp.abs(fresh).reshape(step // 8, 8, tile), axis=0)
        sum_tile[...] = jnp.sum(total, axis=0, keepdims=True)

    pltpu.emit_pipeline(
        add_up,
        grid=(w_ref.shape[1] // tile,),
        in_specs=[
            pl.BlockSpec((rows, tile), lambda j: (0, j)),
            pl.BlockSpec((rank, tile), lambda j: (0, j)),
        ],
        out_specs=[pl.BlockSpec((1, tile), lambda j: (0, j))],
    )(w_ref, high_ref, mine_ref)

    own_small = pltpu.make_async_copy(small_ref, all_ref.at[me, z], own_sem.at[2])
    own_small.start()
    own_part = pltpu.make_async_copy(mine_ref.at[:, columns(me)], parts_ref.at[me], own_sem.at[3])
    own_part.start()
    for k in chips:
        small_copy(k).start()
    for k in order:
        part_copy(k).start()
    for q in range(1, depth):
        for k in near:
            big_copy(k, q).start()
    for q in range(depth):
        for k in late:
            big_copy(k, q).start()
    for u in range(units - held_back):
        unit_copy(u).start()

    @pl.when(me % 2 == 1)
    def _():
        for u in range(units - held_back, units):
            unit_copy(u).start()

    own_small.wait()
    for k in [0] + chips:
        if k:
            small_copy(k).wait()
        for j in range(1, depth):
            far_copy(k, j).start()
    for k in [0] + chips:
        for j in range(1, depth):
            far_copy(k, j).wait()
        pair_copy(k).start()
    own_part.wait()
    for k in order:
        part_copy(k).wait()
    scale = jnp.sum(parts_ref[...], axis=0) / inner
    scale_ref[...] = scale
    inverse = 1.0 / scale
    for k in [0] + chips:
        pair_copy(k).wait()
    own_high.wait()
    own_block.wait()

    for d in range(n):
        for q in range(depth):
            i = d * depth + q
            norm_ref[i * 8:(i + 1) * 8, :] = all_ref[d, q, rank:, :]

    def finish_rows(d, q, r):
        here = pl.ds(pl.multiple_of(d * rows + q * part + r, height), height)
        for c in range(0, cols, width):
            fresh = out_ref[here, c:c + width].astype(jnp.float32) + contract_first(
                all_ref[d, q, :rank, r:r + height], high_own[:, c:c + width]
            )
            out_ref[here, c:c + width] = (fresh * inverse[:, c:c + width]).astype(jnp.bfloat16)

    def finish(k):
        def piece(q, carry):
            if k:
                big_copy(k, q).wait_recv()
            for r in range(0, part, height):
                finish_rows(me ^ k, q, r)
            return carry

        return piece

    for k in [0] + near:
        lax.fori_loop(0, depth, finish(k), 0)
    late_pieces = [finish(k) for k in late]

    def late_round(q, carry):
        for piece in late_pieces:
            piece(q, carry)
        return carry

    lax.fori_loop(0, depth, late_round, 0)
    per = part // height

    def finish_unit(u):
        unit_copy(u).wait_recv()
        finish_rows(me ^ far, u // per, u % per * height)

    for i in range(held_back):
        u = units - held_back + i
        low_late_ref[:, i * height:(i + 1) * height] = all_ref[
            me ^ far, u // per, :rank, u % per * height:u % per * height + height
        ]
    for u in range(units - held_back):
        finish_unit(u)
    for k in near + late:
        for q in range(depth):
            big_copy(k, q).wait_send()
    for u in range(units - held_back):
        unit_copy(u).wait_send()

    @pl.when(me % 2 == 1)
    def _():
        for u in range(units - held_back, units):
            finish_unit(u)
        for u in range(units - held_back, units):
            unit_copy(u).wait_send()


def second_kernel(n, held_back, w_ref, low_ref, high_ref, scale_ref, got_ref, high_own, send_sem, recv_sem, own_sem):
    me = lax.axis_index("shard")
    rows = w_ref.shape[0]
    cols = got_ref.shape[1]
    height = got_ref.shape[0] // held_back
    width = tile_of(cols, 512)
    units = rows // height
    far = n - 2

    def columns(p):
        return pl.ds(pl.multiple_of(p * cols, cols), cols)

    def unit_copy(i):
        u = units - held_back + i
        return pltpu.make_async_remote_copy(
            src_ref=w_ref.at[u * height:(u + 1) * height, columns(me ^ far)],
            dst_ref=got_ref.at[i * height:(i + 1) * height, :],
            send_sem=send_sem.at[i], recv_sem=recv_sem.at[i],
            device_id={"shard": me ^ far}, device_id_type=MESH,
        )

    @pl.when(me % 2 == 0)
    def _():
        barrier = pltpu.get_barrier_semaphore()
        pl.semaphore_signal(barrier, inc=1, device_id={"shard": me ^ far}, device_id_type=MESH)
        own_high = pltpu.make_async_copy(high_ref.at[:, columns(me)], high_own, own_sem)
        own_high.start()
        pl.semaphore_wait(barrier, 1)
        for i in range(held_back):
            unit_copy(i).start()
        inverse = 1.0 / scale_ref[...]
        own_high.wait()
        for i in range(held_back):
            unit_copy(i).wait_recv()
            here = slice(i * height, (i + 1) * height)
            for c in range(0, cols, width):
                fresh = got_ref[here, c:c + width].astype(jnp.float32) + contract_first(
                    low_ref[:, here], high_own[:, c:c + width]
                )
                got_ref[here, c:c + width] = (fresh * inverse[:, c:c + width]).astype(jnp.bfloat16)
        for i in range(held_back):
            unit_copy(i).wait_send()


def put_kernel(held_ref, out_ref, sems):
    pieces = sems.shape[0]
    size = held_ref.shape[0] // pieces
    copies = [
        pltpu.make_async_copy(held_ref.at[i * size:(i + 1) * size, :], out_ref.at[i * size:(i + 1) * size, :], sems.at[i])
        for i in range(pieces)
    ]
    for copy in copies:
        copy.start()
    for copy in copies:
        copy.wait()


def tail_kernel(n, put_ref, got_ref, scale_in, norm_in, out_ref, scale_ref, norm_ref, sem):
    me = lax.axis_index("shard")
    late = got_ref.shape[0]
    rows = out_ref.shape[0] // n
    last = pl.ds(pl.multiple_of((me ^ (n - 2)) * rows + (rows - late), 8), late)
    copy = pltpu.make_async_copy(got_ref, out_ref.at[last, :], sem)

    @pl.when(me % 2 == 0)
    def _():
        copy.start()

    scale_ref[...] = scale_in[...].reshape(scale_ref.shape)
    part = norm_in.shape[1]
    for i in range(norm_in.shape[0] // 8):
        norm_ref[i * part:(i + 1) * part] = norm_in[i * 8:i * 8 + 1, :].reshape(part)

    @pl.when(me % 2 == 0)
    def _():
        copy.wait()


def solution(mesh):
    n, depth = mesh.shape["shard"], mesh.shape["width"]

    def per_device(w_up, low_up, high_up, norm_train, norm_step):
        rows, wide = w_up.shape
        rank = low_up.shape[1]
        cols = wide // n
        part = rows // depth
        height = tile_of(part, 128)
        units = rows // height
        held_back = units // 3
        any_spec = pl.BlockSpec(memory_space=pl.ANY)
        vmem_spec = pl.BlockSpec(memory_space=pltpu.VMEM)
        dma = pltpu.SemaphoreType.DMA
        held, _, scale, norm, low_late = pl.pallas_call(
            functools.partial(exchange_kernel, n, depth, held_back, n * rows),
            out_shape=(
                pltpu.VMEM((n * rows, cols), jnp.bfloat16),
                jax.ShapeDtypeStruct((1, wide), jnp.float32),
                jax.ShapeDtypeStruct((1, cols), jnp.float32),
                jax.ShapeDtypeStruct((n * depth * 8, part), jnp.bfloat16),
                jax.ShapeDtypeStruct((rank, held_back * height), jnp.bfloat16),
            ),
            in_specs=[any_spec, vmem_spec, any_spec, vmem_spec, vmem_spec],
            out_specs=(vmem_spec, any_spec, vmem_spec, vmem_spec, vmem_spec),
            scratch_shapes=[
                pltpu.VMEM((rank + 8, part), jnp.bfloat16),
                pltpu.VMEM((n, depth, rank + 8, part), jnp.bfloat16),
                pltpu.VMEM((n, 1, cols), jnp.float32),
                pltpu.VMEM((rank, cols), jnp.bfloat16),
                dma((n, depth)), dma((n, depth)), dma((n,)), dma((n,)), dma((n, depth)), dma((n, depth)),
                dma((n,)), dma((n,)), dma((n,)), dma((n,)), dma((units,)), dma((units,)), dma((4,)),
            ],
            compiler_params=pltpu.CompilerParams(collective_id=0, has_side_effects=True, vmem_limit_bytes=24 * 2**20),
            name="exchange",
        )(w_up, low_up.T, high_up, norm_train, norm_step)
        serve_up = pl.pallas_call(
            put_kernel,
            out_shape=jax.ShapeDtypeStruct((n * rows, cols), jnp.bfloat16),
            in_specs=[vmem_spec],
            out_specs=any_spec,
            scratch_shapes=[dma((8,))],
            compiler_params=pltpu.CompilerParams(vmem_limit_bytes=4 * 2**20),
            name="put",
        )(held)
        serve_up, scale, norm, low_late = lax.optimization_barrier((serve_up, scale, norm, low_late))
        got = pl.pallas_call(
            functools.partial(second_kernel, n, held_back),
            out_shape=pltpu.VMEM((held_back * height, cols), jnp.bfloat16),
            in_specs=[any_spec, vmem_spec, any_spec, vmem_spec],
            out_specs=vmem_spec,
            scratch_shapes=[
                pltpu.VMEM((rank, cols), jnp.bfloat16), dma((held_back,)), dma((held_back,)), dma,
            ],
            compiler_params=pltpu.CompilerParams(
                collective_id=1, has_side_effects=True, vmem_limit_bytes=16 * 2**20
            ),
            name="second",
        )(w_up, low_late, high_up, scale)
        serve_up, scale_up, serve_norm = pl.pallas_call(
            functools.partial(tail_kernel, n),
            out_shape=(
                jax.ShapeDtypeStruct((n * rows, cols), jnp.bfloat16),
                jax.ShapeDtypeStruct((cols,), jnp.float32),
                jax.ShapeDtypeStruct((n * rows,), jnp.bfloat16),
            ),
            in_specs=[any_spec, vmem_spec, vmem_spec, vmem_spec],
            out_specs=(any_spec, vmem_spec, vmem_spec),
            scratch_shapes=[dma],
            input_output_aliases={0: 0},
            compiler_params=pltpu.CompilerParams(vmem_limit_bytes=8 * 2**20),
            name="tail",
        )(serve_up, got, scale, norm)
        return serve_up, scale_up, serve_norm

    placed = (
        P("shard", "width"),
        P("shard", None),
        P(None, "width"),
        P(("shard", "width")),
        P(("shard", "width")),
    )
    return jax.shard_map(
        per_device,
        mesh=mesh,
        in_specs=placed,
        out_specs=(P(None, ("width", "shard")), P(("width", "shard")), P()),
        check_vma=False,
    )
```

```python
import functools

import jax
import jax.numpy as jnp
from jax import lax
from jax.experimental import pallas as pl
from jax.experimental.pallas import tpu as pltpu
from jax.sharding import PartitionSpec as P

MESH = pl.DeviceIdType.MESH

mix_rate = 0.5


def tile_of(extent, most):
    for size in range(most, 0, -128):
        if extent % size == 0:
            return size
    return extent


def contract_first(a, b):
    return lax.dot_general(a, b, (((0,), (0,)), ((), ())), preferred_element_type=jnp.float32)


def exchange_kernel(
    n, depth, held_back, inner, w_ref, low_in, high_ref, train_in, step_in,
    out_ref, mine_ref, scale_ref, norm_ref, low_late_ref,
    low_ref, train_ref, step_ref, small_ref, all_ref, parts_ref, high_own,
    big_send, big_recv, small_send, small_recv, far_send, far_recv,
    pair_send, pair_recv, part_send, part_recv, unit_send, unit_recv, own_sem,
):
    me = lax.axis_index("shard")
    z = lax.axis_index("width")
    rows = w_ref.shape[0]
    rank = low_ref.shape[0]
    cols = out_ref.shape[1]
    part = rows // depth
    height = tile_of(part, 128)
    width = tile_of(cols, 512)
    units = rows // height
    far = n - 2
    order = sorted(range(1, n), key=lambda k: (bin(k >> 1).count("1"), k))
    near = [k for k in order if bin(k >> 1).count("1") < 2]
    late = [k for k in order if bin(k >> 1).count("1") >= 2 and k != far]
    chips = [k for k in order if k % 2 == 0]

    def columns(p):
        return pl.ds(pl.multiple_of(p * cols, cols), cols)

    def rows_of(p, q):
        return pl.ds(pl.multiple_of(p * rows + q * part, part), part)

    def big_copy(k, q):
        return pltpu.make_async_remote_copy(
            src_ref=w_ref.at[pl.ds(pl.multiple_of(q * part, part), part), columns(me ^ k)],
            dst_ref=out_ref.at[rows_of(me, q), :],
            send_sem=big_send.at[k, q], recv_sem=big_recv.at[k, q],
            device_id={"shard": me ^ k}, device_id_type=MESH,
        )

    def unit_copy(u):
        return pltpu.make_async_remote_copy(
            src_ref=w_ref.at[u * height:(u + 1) * height, columns(me ^ far)],
            dst_ref=out_ref.at[pl.ds(pl.multiple_of(me * rows + u * height, height), height), :],
            send_sem=unit_send.at[u], recv_sem=unit_recv.at[u],
            device_id={"shard": me ^ far}, device_id_type=MESH,
        )

    def small_copy(k):
        return pltpu.make_async_remote_copy(
            src_ref=small_ref, dst_ref=all_ref.at[me, z],
            send_sem=small_send.at[k], recv_sem=small_recv.at[k],
            device_id={"shard": me ^ k}, device_id_type=MESH,
        )

    def far_copy(k, j):
        return pltpu.make_async_remote_copy(
            src_ref=all_ref.at[me ^ k, z], dst_ref=all_ref.at[me ^ k, z],
            send_sem=far_send.at[k, j], recv_sem=far_recv.at[k, j],
            device_id={"width": z ^ j}, device_id_type=MESH,
        )

    def pair_copy(k):
        return pltpu.make_async_remote_copy(
            src_ref=all_ref.at[me ^ k], dst_ref=all_ref.at[me ^ k],
            send_sem=pair_send.at[k], recv_sem=pair_recv.at[k],
            device_id={"shard": me ^ 1}, device_id_type=MESH,
        )

    def part_copy(k):
        return pltpu.make_async_remote_copy(
            src_ref=mine_ref.at[:, columns(me ^ k)], dst_ref=parts_ref.at[me],
            send_sem=part_send.at[k], recv_sem=part_recv.at[k],
            device_id={"shard": me ^ k}, device_id_type=MESH,
        )

    barrier = pltpu.get_barrier_semaphore()
    for k in order:
        pl.semaphore_signal(barrier, inc=1, device_id={"shard": me ^ k}, device_id_type=MESH)
    for j in range(1, depth):
        pl.semaphore_signal(barrier, inc=1, device_id={"width": z ^ j}, device_id_type=MESH)
    taken = [
        pltpu.make_async_copy(low_in, low_ref, own_sem.at[4]),
        pltpu.make_async_copy(train_in, train_ref, own_sem.at[5]),
        pltpu.make_async_copy(step_in, step_ref, own_sem.at[6]),
    ]
    for copy in taken:
        copy.start()
    pl.semaphore_wait(barrier, len(order) + depth - 1)

    for q in range(1):
        for k in near:
            big_copy(k, q).start()

    own_block = pltpu.make_async_copy(
        w_ref.at[:, columns(me)], out_ref.at[pl.ds(pl.multiple_of(me * rows, rows), rows), :], own_sem.at[0]
    )
    own_block.start()
    own_high = pltpu.make_async_copy(high_ref.at[:, columns(me)], high_own, own_sem.at[1])
    own_high.start()

    for copy in taken:
        copy.wait()
    for j in range(depth):
        @pl.when(z == j)
        def _():
            small_ref[:rank, :] = low_ref[:, j * part:(j + 1) * part] * jnp.bfloat16(mix_rate)
    gain = (train_ref[...] + step_ref[...]).reshape(1, part)
    small_ref[rank:, :] = jnp.broadcast_to(gain, (8, part)).astype(jnp.bfloat16)

    tile = tile_of(w_ref.shape[1], 512)
    step = tile_of(rows, 256)

    def add_up(w_tile, high_tile, sum_tile):
        total = jnp.zeros((8, tile), jnp.float32)
        for r in range(0, rows, step):
            fresh = w_tile[r:r + step, :].astype(jnp.float32) + mix_rate * contract_first(
                low_ref[:, r:r + step], high_tile[...]
            )
            total = total + jnp.sum(jnp.abs(fresh).reshape(step // 8, 8, tile), axis=0)
        sum_tile[...] = jnp.sum(total, axis=0, keepdims=True)

    pltpu.emit_pipeline(
        add_up,
        grid=(w_ref.shape[1] // tile,),
        in_specs=[
            pl.BlockSpec((rows, tile), lambda j: (0, j)),
            pl.BlockSpec((rank, tile), lambda j: (0, j)),
        ],
        out_specs=[pl.BlockSpec((1, tile), lambda j: (0, j))],
    )(w_ref, high_ref, mine_ref)

    own_small = pltpu.make_async_copy(small_ref, all_ref.at[me, z], own_sem.at[2])
    own_small.start()
    own_part = pltpu.make_async_copy(mine_ref.at[:, columns(me)], parts_ref.at[me], own_sem.at[3])
    own_part.start()
    for k in chips:
        small_copy(k).start()
    for k in order:
        part_copy(k).start()
    for q in range(1, depth):
        for k in near:
            big_copy(k, q).start()
    for q in range(depth):
        for k in late:
            big_copy(k, q).start()
    for u in range(units - held_back):
        unit_copy(u).start()

    @pl.when(me % 2 == 1)
    def _():
        for u in range(units - held_back, units):
            unit_copy(u).start()

    own_small.wait()
    for k in [0] + chips:
        if k:
            small_copy(k).wait()
        for j in range(1, depth):
            far_copy(k, j).start()
    for k in [0] + chips:
        for j in range(1, depth):
            far_copy(k, j).wait()
        pair_copy(k).start()
    own_part.wait()
    for k in order:
        part_copy(k).wait()
    scale = jnp.sum(parts_ref[...], axis=0) / inner
    scale_ref[...] = scale
    inverse = 1.0 / scale
    for k in [0] + chips:
        pair_copy(k).wait()
    own_high.wait()
    own_block.wait()

    for d in range(n):
        for q in range(depth):
            i = d * depth + q
            norm_ref[i * 8:(i + 1) * 8, :] = all_ref[d, q, rank:, :]

    def finish_rows(d, q, r):
        here = pl.ds(pl.multiple_of(d * rows + q * part + r, height), height)
        for c in range(0, cols, width):
            fresh = out_ref[here, c:c + width].astype(jnp.float32) + contract_first(
                all_ref[d, q, :rank, r:r + height], high_own[:, c:c + width]
            )
            out_ref[here, c:c + width] = (fresh * inverse[:, c:c + width]).astype(jnp.bfloat16)

    def finish(k):
        def piece(q, carry):
            if k:
                big_copy(k, q).wait_recv()
            for r in range(0, part, height):
                finish_rows(me ^ k, q, r)
            return carry

        return piece

    for k in [0] + near:
        lax.fori_loop(0, depth, finish(k), 0)
    late_pieces = [finish(k) for k in late]

    def late_round(q, carry):
        for piece in late_pieces:
            piece(q, carry)
        return carry

    lax.fori_loop(0, depth, late_round, 0)
    per = part // height

    def finish_unit(u):
        unit_copy(u).wait_recv()
        finish_rows(me ^ far, u // per, u % per * height)

    for i in range(held_back):
        u = units - held_back + i
        low_late_ref[:, i * height:(i + 1) * height] = all_ref[
            me ^ far, u // per, :rank, u % per * height:u % per * height + height
        ]
    for u in range(units - held_back):
        finish_unit(u)
    for k in near + late:
        for q in range(depth):
            big_copy(k, q).wait_send()
    for u in range(units - held_back):
        unit_copy(u).wait_send()

    @pl.when(me % 2 == 1)
    def _():
        for u in range(units - held_back, units):
            finish_unit(u)
        for u in range(units - held_back, units):
            unit_copy(u).wait_send()


def second_kernel(n, held_back, w_ref, low_ref, high_ref, scale_ref, got_ref, high_own, send_sem, recv_sem, own_sem):
    me = lax.axis_index("shard")
    rows = w_ref.shape[0]
    cols = got_ref.shape[1]
    height = got_ref.shape[0] // held_back
    width = tile_of(cols, 512)
    units = rows // height
    far = n - 2

    def columns(p):
        return pl.ds(pl.multiple_of(p * cols, cols), cols)

    def unit_copy(i):
        u = units - held_back + i
        return pltpu.make_async_remote_copy(
            src_ref=w_ref.at[u * height:(u + 1) * height, columns(me ^ far)],
            dst_ref=got_ref.at[i * height:(i + 1) * height, :],
            send_sem=send_sem.at[i], recv_sem=recv_sem.at[i],
            device_id={"shard": me ^ far}, device_id_type=MESH,
        )

    @pl.when(me % 2 == 0)
    def _():
        barrier = pltpu.get_barrier_semaphore()
        pl.semaphore_signal(barrier, inc=1, device_id={"shard": me ^ far}, device_id_type=MESH)
        own_high = pltpu.make_async_copy(high_ref.at[:, columns(me)], high_own, own_sem)
        own_high.start()
        pl.semaphore_wait(barrier, 1)
        for i in range(held_back):
            unit_copy(i).start()
        inverse = 1.0 / scale_ref[...]
        own_high.wait()
        for i in range(held_back):
            unit_copy(i).wait_recv()
            here = slice(i * height, (i + 1) * height)
            for c in range(0, cols, width):
                fresh = got_ref[here, c:c + width].astype(jnp.float32) + contract_first(
                    low_ref[:, here], high_own[:, c:c + width]
                )
                got_ref[here, c:c + width] = (fresh * inverse[:, c:c + width]).astype(jnp.bfloat16)
        for i in range(held_back):
            unit_copy(i).wait_send()


def put_kernel(held_ref, out_ref, sems):
    pieces = sems.shape[0]
    size = held_ref.shape[0] // pieces
    copies = [
        pltpu.make_async_copy(held_ref.at[i * size:(i + 1) * size, :], out_ref.at[i * size:(i + 1) * size, :], sems.at[i])
        for i in range(pieces)
    ]
    for copy in copies:
        copy.start()
    for copy in copies:
        copy.wait()


def side_kernel(scale_in, norm_in, scale_ref, norm_ref):
    scale_ref[...] = scale_in[...].reshape(scale_ref.shape)
    part = norm_in.shape[1]
    for i in range(norm_in.shape[0] // 8):
        norm_ref[i * part:(i + 1) * part] = norm_in[i * 8:i * 8 + 1, :].reshape(part)


def tail_kernel(n, put_ref, got_ref, out_ref, sem):
    me = lax.axis_index("shard")
    late = got_ref.shape[0]
    rows = out_ref.shape[0] // n
    last = pl.ds(pl.multiple_of((me ^ (n - 2)) * rows + (rows - late), 8), late)

    @pl.when(me % 2 == 0)
    def _():
        copy = pltpu.make_async_copy(got_ref, out_ref.at[last, :], sem)
        copy.start()
        copy.wait()


def solution(mesh):
    n, depth = mesh.shape["shard"], mesh.shape["width"]

    def per_device(w_up, low_up, high_up, norm_train, norm_step):
        rows, wide = w_up.shape
        rank = low_up.shape[1]
        cols = wide // n
        part = rows // depth
        height = tile_of(part, 128)
        units = rows // height
        held_back = max(1, units // 2)
        any_spec = pl.BlockSpec(memory_space=pl.ANY)
        vmem_spec = pl.BlockSpec(memory_space=pltpu.VMEM)
        dma = pltpu.SemaphoreType.DMA
        held, _, scale, norm, low_late = pl.pallas_call(
            functools.partial(exchange_kernel, n, depth, held_back, n * rows),
            out_shape=(
                pltpu.VMEM((n * rows, cols), jnp.bfloat16),
                jax.ShapeDtypeStruct((1, wide), jnp.float32),
                jax.ShapeDtypeStruct((1, cols), jnp.float32),
                jax.ShapeDtypeStruct((n * depth * 8, part), jnp.bfloat16),
                jax.ShapeDtypeStruct((rank, held_back * height), jnp.bfloat16),
            ),
            in_specs=[any_spec] * 5,
            out_specs=(vmem_spec, any_spec, vmem_spec, vmem_spec, vmem_spec),
            scratch_shapes=[
                pltpu.VMEM((rank, rows), jnp.bfloat16),
                pltpu.VMEM((part,), jnp.float32),
                pltpu.VMEM((part,), jnp.float32),
                pltpu.VMEM((rank + 8, part), jnp.bfloat16),
                pltpu.VMEM((n, depth, rank + 8, part), jnp.bfloat16),
                pltpu.VMEM((n, 1, cols), jnp.float32),
                pltpu.VMEM((rank, cols), jnp.bfloat16),
                dma((n, depth)), dma((n, depth)), dma((n,)), dma((n,)), dma((n, depth)), dma((n, depth)),
                dma((n,)), dma((n,)), dma((n,)), dma((n,)), dma((units,)), dma((units,)), dma((7,)),
            ],
            compiler_params=pltpu.CompilerParams(collective_id=0, has_side_effects=True, vmem_limit_bytes=24 * 2**20),
            name="exchange",
        )(w_up, low_up.T, high_up, norm_train, norm_step)
        serve_up = pl.pallas_call(
            put_kernel,
            out_shape=jax.ShapeDtypeStruct((n * rows, cols), jnp.bfloat16),
            in_specs=[vmem_spec],
            out_specs=any_spec,
            scratch_shapes=[dma((8,))],
            compiler_params=pltpu.CompilerParams(vmem_limit_bytes=4 * 2**20),
            name="put",
        )(held)
        serve_up, scale, norm, low_late = lax.optimization_barrier((serve_up, scale, norm, low_late))
        scale_up, serve_norm = pl.pallas_call(
            side_kernel,
            out_shape=(
                jax.ShapeDtypeStruct((cols,), jnp.float32),
                jax.ShapeDtypeStruct((n * rows,), jnp.bfloat16),
            ),
            in_specs=[vmem_spec, vmem_spec],
            out_specs=(vmem_spec, vmem_spec),
            compiler_params=pltpu.CompilerParams(vmem_limit_bytes=4 * 2**20),
            name="side",
        )(scale, norm)
        scale, low_late, scale_up, serve_norm = lax.optimization_barrier((scale, low_late, scale_up, serve_norm))
        got = pl.pallas_call(
            functools.partial(second_kernel, n, held_back),
            out_shape=pltpu.VMEM((held_back * height, cols), jnp.bfloat16),
            in_specs=[any_spec, vmem_spec, any_spec, vmem_spec],
            out_specs=vmem_spec,
            scratch_shapes=[
                pltpu.VMEM((rank, cols), jnp.bfloat16), dma((held_back,)), dma((held_back,)), dma,
            ],
            compiler_params=pltpu.CompilerParams(
                collective_id=1, has_side_effects=True, vmem_limit_bytes=16 * 2**20
            ),
            name="second",
        )(w_up, low_late, high_up, scale)
        serve_up = pl.pallas_call(
            functools.partial(tail_kernel, n),
            out_shape=jax.ShapeDtypeStruct((n * rows, cols), jnp.bfloat16),
            in_specs=[any_spec, vmem_spec],
            out_specs=any_spec,
            scratch_shapes=[dma],
            input_output_aliases={0: 0},
            compiler_params=pltpu.CompilerParams(vmem_limit_bytes=8 * 2**20),
            name="tail",
        )(serve_up, got)
        return serve_up, scale_up, serve_norm

    placed = (
        P("shard", "width"),
        P("shard", None),
        P(None, "width"),
        P(("shard", "width")),
        P(("shard", "width")),
    )
    return jax.shard_map(
        per_device,
        mesh=mesh,
        in_specs=placed,
        out_specs=(P(None, ("width", "shard")), P(("width", "shard")), P()),
        check_vma=False,
    )
```

```python
import functools

import jax
import jax.numpy as jnp
from jax import lax
from jax.experimental import pallas as pl
from jax.experimental.pallas import tpu as pltpu
from jax.sharding import PartitionSpec as P

MESH = pl.DeviceIdType.MESH

mix_rate = 0.5


def tile_of(extent, most):
    for size in range(most, 0, -128):
        if extent % size == 0:
            return size
    return extent


def contract_first(a, b):
    return lax.dot_general(a, b, (((0,), (0,)), ((), ())), preferred_element_type=jnp.float32)


def exchange_kernel(
    n, depth, held_back, inner, w_ref, low_in, high_ref, train_in, step_in,
    out_ref, mine_ref, scale_ref, norm_ref, low_late_ref,
    low_ref, train_ref, step_ref, small_ref, all_ref, parts_ref, high_own,
    big_send, big_recv, small_send, small_recv, far_send, far_recv,
    pair_send, pair_recv, part_send, part_recv, unit_send, unit_recv, own_sem,
):
    me = lax.axis_index("shard")
    z = lax.axis_index("width")
    rows = w_ref.shape[0]
    rank = low_ref.shape[0]
    cols = out_ref.shape[1]
    part = rows // depth
    height = tile_of(part, 128)
    width = tile_of(cols, 512)
    units = rows // height
    far = n - 2
    order = sorted(range(1, n), key=lambda k: (bin(k >> 1).count("1"), k))
    near = [k for k in order if bin(k >> 1).count("1") < 2]
    late = [k for k in order if bin(k >> 1).count("1") >= 2 and k != far]
    chips = [k for k in order if k % 2 == 0]

    def columns(p):
        return pl.ds(pl.multiple_of(p * cols, cols), cols)

    def rows_of(p, q):
        return pl.ds(pl.multiple_of(p * rows + q * part, part), part)

    def big_copy(k, q):
        return pltpu.make_async_remote_copy(
            src_ref=w_ref.at[pl.ds(pl.multiple_of(q * part, part), part), columns(me ^ k)],
            dst_ref=out_ref.at[rows_of(me, q), :],
            send_sem=big_send.at[k, q], recv_sem=big_recv.at[k, q],
            device_id={"shard": me ^ k}, device_id_type=MESH,
        )

    def unit_copy(u):
        return pltpu.make_async_remote_copy(
            src_ref=w_ref.at[u * height:(u + 1) * height, columns(me ^ far)],
            dst_ref=out_ref.at[pl.ds(pl.multiple_of(me * rows + u * height, height), height), :],
            send_sem=unit_send.at[u], recv_sem=unit_recv.at[u],
            device_id={"shard": me ^ far}, device_id_type=MESH,
        )

    def small_copy(k):
        return pltpu.make_async_remote_copy(
            src_ref=small_ref, dst_ref=all_ref.at[me, z],
            send_sem=small_send.at[k], recv_sem=small_recv.at[k],
            device_id={"shard": me ^ k}, device_id_type=MESH,
        )

    def far_copy(k, j):
        return pltpu.make_async_remote_copy(
            src_ref=all_ref.at[me ^ k, z], dst_ref=all_ref.at[me ^ k, z],
            send_sem=far_send.at[k, j], recv_sem=far_recv.at[k, j],
            device_id={"width": z ^ j}, device_id_type=MESH,
        )

    def pair_copy(k):
        return pltpu.make_async_remote_copy(
            src_ref=all_ref.at[me ^ k], dst_ref=all_ref.at[me ^ k],
            send_sem=pair_send.at[k], recv_sem=pair_recv.at[k],
            device_id={"shard": me ^ 1}, device_id_type=MESH,
        )

    def part_copy(k):
        return pltpu.make_async_remote_copy(
            src_ref=mine_ref.at[:, columns(me ^ k)], dst_ref=parts_ref.at[me],
            send_sem=part_send.at[k], recv_sem=part_recv.at[k],
            device_id={"shard": me ^ k}, device_id_type=MESH,
        )

    barrier = pltpu.get_barrier_semaphore()
    for k in order:
        pl.semaphore_signal(barrier, inc=1, device_id={"shard": me ^ k}, device_id_type=MESH)
    for j in range(1, depth):
        pl.semaphore_signal(barrier, inc=1, device_id={"width": z ^ j}, device_id_type=MESH)
    taken = [
        pltpu.make_async_copy(low_in, low_ref, own_sem.at[4]),
        pltpu.make_async_copy(train_in, train_ref, own_sem.at[5]),
        pltpu.make_async_copy(step_in, step_ref, own_sem.at[6]),
    ]
    for copy in taken:
        copy.start()
    pl.semaphore_wait(barrier, len(order) + depth - 1)

    for q in range(1):
        for k in near:
            big_copy(k, q).start()

    own_block = pltpu.make_async_copy(
        w_ref.at[:, columns(me)], out_ref.at[pl.ds(pl.multiple_of(me * rows, rows), rows), :], own_sem.at[0]
    )
    own_block.start()
    own_high = pltpu.make_async_copy(high_ref.at[:, columns(me)], high_own, own_sem.at[1])
    own_high.start()

    for copy in taken:
        copy.wait()
    for j in range(depth):
        @pl.when(z == j)
        def _():
            small_ref[:rank, :] = low_ref[:, j * part:(j + 1) * part] * jnp.bfloat16(mix_rate)
    gain = (train_ref[...] + step_ref[...]).reshape(1, part)
    small_ref[rank:, :] = jnp.broadcast_to(gain, (8, part)).astype(jnp.bfloat16)

    tile = tile_of(w_ref.shape[1], 512)
    step = tile_of(rows, 256)

    def add_up(w_tile, high_tile, sum_tile):
        total = jnp.zeros((8, tile), jnp.float32)
        for r in range(0, rows, step):
            fresh = w_tile[r:r + step, :].astype(jnp.float32) + mix_rate * contract_first(
                low_ref[:, r:r + step], high_tile[...]
            )
            total = total + jnp.sum(jnp.abs(fresh).reshape(step // 8, 8, tile), axis=0)
        sum_tile[...] = jnp.sum(total, axis=0, keepdims=True)

    pltpu.emit_pipeline(
        add_up,
        grid=(w_ref.shape[1] // tile,),
        in_specs=[
            pl.BlockSpec((rows, tile), lambda j: (0, j)),
            pl.BlockSpec((rank, tile), lambda j: (0, j)),
        ],
        out_specs=[pl.BlockSpec((1, tile), lambda j: (0, j))],
    )(w_ref, high_ref, mine_ref)

    own_small = pltpu.make_async_copy(small_ref, all_ref.at[me, z], own_sem.at[2])
    own_small.start()
    own_part = pltpu.make_async_copy(mine_ref.at[:, columns(me)], parts_ref.at[me], own_sem.at[3])
    own_part.start()
    for k in chips:
        small_copy(k).start()
    for k in order:
        part_copy(k).start()
    for q in range(1, depth):
        for k in near:
            big_copy(k, q).start()
    for q in range(depth):
        for k in late:
            big_copy(k, q).start()
    for u in range(units - held_back):
        unit_copy(u).start()

    @pl.when(me % 2 == 0)
    def _():
        for u in range(units - held_back, units):
            unit_copy(u).start()

    own_small.wait()
    for k in [0] + chips:
        if k:
            small_copy(k).wait()
        for j in range(1, depth):
            far_copy(k, j).start()
    for k in [0] + chips:
        for j in range(1, depth):
            far_copy(k, j).wait()
        pair_copy(k).start()
    own_part.wait()
    for k in order:
        part_copy(k).wait()
    scale = jnp.sum(parts_ref[...], axis=0) / inner
    scale_ref[...] = scale
    inverse = 1.0 / scale
    for k in [0] + chips:
        pair_copy(k).wait()
    own_high.wait()
    own_block.wait()

    for d in range(n):
        for q in range(depth):
            i = d * depth + q
            norm_ref[i * 8:(i + 1) * 8, :] = all_ref[d, q, rank:, :]

    def finish_rows(d, q, r):
        here = pl.ds(pl.multiple_of(d * rows + q * part + r, height), height)
        for c in range(0, cols, width):
            fresh = out_ref[here, c:c + width].astype(jnp.float32) + contract_first(
                all_ref[d, q, :rank, r:r + height], high_own[:, c:c + width]
            )
            out_ref[here, c:c + width] = (fresh * inverse[:, c:c + width]).astype(jnp.bfloat16)

    def finish(k):
        def piece(q, carry):
            if k:
                big_copy(k, q).wait_recv()
            for r in range(0, part, height):
                finish_rows(me ^ k, q, r)
            return carry

        return piece

    for k in [0] + near:
        lax.fori_loop(0, depth, finish(k), 0)
    late_pieces = [finish(k) for k in late]

    def late_round(q, carry):
        for piece in late_pieces:
            piece(q, carry)
        return carry

    lax.fori_loop(0, depth, late_round, 0)
    per = part // height

    def finish_unit(u):
        unit_copy(u).wait_recv()
        finish_rows(me ^ far, u // per, u % per * height)

    for i in range(held_back):
        u = units - held_back + i
        low_late_ref[:, i * height:(i + 1) * height] = all_ref[
            me ^ far, u // per, :rank, u % per * height:u % per * height + height
        ]
    for u in range(units - held_back):
        finish_unit(u)
    for k in near + late:
        for q in range(depth):
            big_copy(k, q).wait_send()
    for u in range(units - held_back):
        unit_copy(u).wait_send()

    @pl.when(me % 2 == 0)
    def _():
        for u in range(units - held_back, units):
            finish_unit(u)
        for u in range(units - held_back, units):
            unit_copy(u).wait_send()


def second_kernel(n, held_back, w_ref, low_ref, high_ref, scale_ref, got_ref, high_own, send_sem, recv_sem, own_sem):
    me = lax.axis_index("shard")
    rows = w_ref.shape[0]
    cols = got_ref.shape[1]
    height = got_ref.shape[0] // held_back
    width = tile_of(cols, 512)
    units = rows // height
    far = n - 2

    def columns(p):
        return pl.ds(pl.multiple_of(p * cols, cols), cols)

    def unit_copy(i):
        u = units - held_back + i
        return pltpu.make_async_remote_copy(
            src_ref=w_ref.at[u * height:(u + 1) * height, columns(me ^ far)],
            dst_ref=got_ref.at[i * height:(i + 1) * height, :],
            send_sem=send_sem.at[i], recv_sem=recv_sem.at[i],
            device_id={"shard": me ^ far}, device_id_type=MESH,
        )

    @pl.when(me % 2 == 1)
    def _():
        barrier = pltpu.get_barrier_semaphore()
        pl.semaphore_signal(barrier, inc=1, device_id={"shard": me ^ far}, device_id_type=MESH)
        own_high = pltpu.make_async_copy(high_ref.at[:, columns(me)], high_own, own_sem)
        own_high.start()
        pl.semaphore_wait(barrier, 1)
        for i in range(held_back):
            unit_copy(i).start()
        inverse = 1.0 / scale_ref[...]
        own_high.wait()
        for i in range(held_back):
            unit_copy(i).wait_recv()
            here = slice(i * height, (i + 1) * height)
            for c in range(0, cols, width):
                fresh = got_ref[here, c:c + width].astype(jnp.float32) + contract_first(
                    low_ref[:, here], high_own[:, c:c + width]
                )
                got_ref[here, c:c + width] = (fresh * inverse[:, c:c + width]).astype(jnp.bfloat16)
        for i in range(held_back):
            unit_copy(i).wait_send()


def put_kernel(held_ref, out_ref, sems):
    pieces = sems.shape[0]
    size = held_ref.shape[0] // pieces
    copies = [
        pltpu.make_async_copy(held_ref.at[i * size:(i + 1) * size, :], out_ref.at[i * size:(i + 1) * size, :], sems.at[i])
        for i in range(pieces)
    ]
    for copy in copies:
        copy.start()
    for copy in copies:
        copy.wait()


def side_kernel(scale_in, norm_in, scale_ref, norm_ref):
    scale_ref[...] = scale_in[...].reshape(scale_ref.shape)
    part = norm_in.shape[1]
    for i in range(norm_in.shape[0] // 8):
        norm_ref[i * part:(i + 1) * part] = norm_in[i * 8:i * 8 + 1, :].reshape(part)


def tail_kernel(n, put_ref, got_ref, out_ref, sem):
    me = lax.axis_index("shard")
    late = got_ref.shape[0]
    rows = out_ref.shape[0] // n
    last = pl.ds(pl.multiple_of((me ^ (n - 2)) * rows + (rows - late), 8), late)

    @pl.when(me % 2 == 1)
    def _():
        copy = pltpu.make_async_copy(got_ref, out_ref.at[last, :], sem)
        copy.start()
        copy.wait()


def solution(mesh):
    n, depth = mesh.shape["shard"], mesh.shape["width"]

    def per_device(w_up, low_up, high_up, norm_train, norm_step):
        rows, wide = w_up.shape
        rank = low_up.shape[1]
        cols = wide // n
        part = rows // depth
        height = tile_of(part, 128)
        units = rows // height
        held_back = max(1, units // 2)
        any_spec = pl.BlockSpec(memory_space=pl.ANY)
        vmem_spec = pl.BlockSpec(memory_space=pltpu.VMEM)
        dma = pltpu.SemaphoreType.DMA
        held, _, scale, norm, low_late = pl.pallas_call(
            functools.partial(exchange_kernel, n, depth, held_back, n * rows),
            out_shape=(
                pltpu.VMEM((n * rows, cols), jnp.bfloat16),
                jax.ShapeDtypeStruct((1, wide), jnp.float32),
                jax.ShapeDtypeStruct((1, cols), jnp.float32),
                jax.ShapeDtypeStruct((n * depth * 8, part), jnp.bfloat16),
                jax.ShapeDtypeStruct((rank, held_back * height), jnp.bfloat16),
            ),
            in_specs=[any_spec] * 5,
            out_specs=(vmem_spec, any_spec, vmem_spec, vmem_spec, vmem_spec),
            scratch_shapes=[
                pltpu.VMEM((rank, rows), jnp.bfloat16),
                pltpu.VMEM((part,), jnp.float32),
                pltpu.VMEM((part,), jnp.float32),
                pltpu.VMEM((rank + 8, part), jnp.bfloat16),
                pltpu.VMEM((n, depth, rank + 8, part), jnp.bfloat16),
                pltpu.VMEM((n, 1, cols), jnp.float32),
                pltpu.VMEM((rank, cols), jnp.bfloat16),
                dma((n, depth)), dma((n, depth)), dma((n,)), dma((n,)), dma((n, depth)), dma((n, depth)),
                dma((n,)), dma((n,)), dma((n,)), dma((n,)), dma((units,)), dma((units,)), dma((7,)),
            ],
            compiler_params=pltpu.CompilerParams(collective_id=0, has_side_effects=True, vmem_limit_bytes=24 * 2**20),
            name="exchange",
        )(w_up, low_up.T, high_up, norm_train, norm_step)
        serve_up = pl.pallas_call(
            put_kernel,
            out_shape=jax.ShapeDtypeStruct((n * rows, cols), jnp.bfloat16),
            in_specs=[vmem_spec],
            out_specs=any_spec,
            scratch_shapes=[dma((8,))],
            compiler_params=pltpu.CompilerParams(vmem_limit_bytes=4 * 2**20),
            name="put",
        )(held)
        serve_up, scale, norm, low_late = lax.optimization_barrier((serve_up, scale, norm, low_late))
        scale_up, serve_norm = pl.pallas_call(
            side_kernel,
            out_shape=(
                jax.ShapeDtypeStruct((cols,), jnp.float32),
                jax.ShapeDtypeStruct((n * rows,), jnp.bfloat16),
            ),
            in_specs=[vmem_spec, vmem_spec],
            out_specs=(vmem_spec, vmem_spec),
            compiler_params=pltpu.CompilerParams(vmem_limit_bytes=4 * 2**20),
            name="side",
        )(scale, norm)
        scale, low_late, scale_up, serve_norm = lax.optimization_barrier((scale, low_late, scale_up, serve_norm))
        got = pl.pallas_call(
            functools.partial(second_kernel, n, held_back),
            out_shape=pltpu.VMEM((held_back * height, cols), jnp.bfloat16),
            in_specs=[any_spec, vmem_spec, any_spec, vmem_spec],
            out_specs=vmem_spec,
            scratch_shapes=[
                pltpu.VMEM((rank, cols), jnp.bfloat16), dma((held_back,)), dma((held_back,)), dma,
            ],
            compiler_params=pltpu.CompilerParams(
                collective_id=1, has_side_effects=True, vmem_limit_bytes=16 * 2**20
            ),
            name="second",
        )(w_up, low_late, high_up, scale)
        serve_up = pl.pallas_call(
            functools.partial(tail_kernel, n),
            out_shape=jax.ShapeDtypeStruct((n * rows, cols), jnp.bfloat16),
            in_specs=[any_spec, vmem_spec],
            out_specs=any_spec,
            scratch_shapes=[dma],
            input_output_aliases={0: 0},
            compiler_params=pltpu.CompilerParams(vmem_limit_bytes=8 * 2**20),
            name="tail",
        )(serve_up, got)
        return serve_up, scale_up, serve_norm

    placed = (
        P("shard", "width"),
        P("shard", None),
        P(None, "width"),
        P(("shard", "width")),
        P(("shard", "width")),
    )
    return jax.shard_map(
        per_device,
        mesh=mesh,
        in_specs=placed,
        out_specs=(P(None, ("width", "shard")), P(("width", "shard")), P()),
        check_vma=False,
    )
```
